32 devices in a mesh: section: 4 (over z), expert: 8 (over y, x, core).
Axes of the slice: x: 2, y: 2, z: 4, core: 2. Of those that a mesh axis runs over, the one named last changes fastest.
Arguments:
- tokens: bfloat16 [4, 1, 128, 1024], P(None, None, 'expert'), may hold values from -6 to 6
- expert_ids: int32 [4, 4, 1, 128, 2], P('section', None, None, 'expert'), may hold values from 0 to 7, as said below
- router_weight: float32 [4, 1, 1024, 8], P('section'), may hold values from -0.375 to 0.375
- w_gate: bfloat16 [4, 8, 1024, 1792], P('section', 'expert'), may hold values from -0.1875 to 0.1875
- w_up: bfloat16 [4, 8, 1024, 1792], P('section', 'expert'), may hold values from -0.1875 to 0.1875
- w_down: bfloat16 [4, 8, 1792, 1024], P('section', 'expert'), may hold values from -0.125 to 0.125
Outputs:
- layer_outputs: bfloat16 [4, 4, 1, 128, 1024], P('section', None, None, 'expert')
The draws below stay inside these ranges and needn't reach their ends.
Inputs may be any that keep to these rules, and one draw needn't show every extreme that they name: `expert_ids`: the two entries of a token are different experts. In each aligned block of 8 tokens (same layer, micro-batch and replica) no expert is named by more than 4 tokens, and some expert by exactly 4.
All inputs are finite; a program needn't handle non-finite values.
Results may differ from the reference program's by a relative error of at most 0.02.
Values may be sent and summed in bfloat16 or wider, within the bound.
No kernel may reach another device: no remote copies, remote signals or barrier semaphores. Data moves between devices by JAX's collectives and lax.ppermute only.
A program may use at most 64 MiB of HBM per device.

```python
import jax
import jax.numpy as jnp
from jax import lax

D = 1024
FF = 1792
EXPERTS = 8
TOP = 2
TOK_DEV = 16
MICRO = 4
CAP = 4
REPS = 1
TOKENS = 128
LAYERS = 4
N_EXPERT = 8


def route_block(block_key, hot_expert, aligned):
    keys = jax.random.split(block_key, 5)
    block_rows = TOK_DEV // 2
    positions = jnp.arange(EXPERTS, dtype=jnp.int32)
    ordering = jax.random.permutation(keys[0], EXPERTS).astype(jnp.int32)
    moved = jnp.where(ordering == hot_expert, ordering[0], jnp.where(positions == 0, hot_expert, ordering))
    ordering = jnp.where(aligned, moved, ordering).astype(jnp.int32)
    double_full = jax.random.randint(keys[1], (), 0, 2, dtype=jnp.int32)
    ticket_count = EXPERTS * CAP
    labels = (jnp.arange(ticket_count, dtype=jnp.int32) // CAP).astype(jnp.int32)
    shuffled = jax.random.permutation(keys[2], ticket_count).astype(jnp.int32)
    ranking = jnp.argsort(shuffled, stable=True).astype(jnp.int32)
    forced = jnp.logical_or(labels == 0, jnp.logical_and(labels == 1, double_full == 1)).astype(jnp.int32)
    priority = (ranking + forced * ticket_count).astype(jnp.int32)
    selected = jnp.argsort(-priority, stable=True)[:2 * block_rows].astype(jnp.int32)
    picked = jnp.sort(labels[selected])
    named = ordering[picked]
    pairs = jnp.stack([named[:block_rows], named[block_rows:]], axis=-1)
    flips = jax.random.randint(keys[3], (block_rows, 1), 0, 2, dtype=jnp.int32)
    pairs = jnp.where(flips == 1, pairs[:, ::-1], pairs)
    rows_order = jax.random.permutation(keys[4], block_rows).astype(jnp.int32)
    return pairs[rows_order].astype(jnp.int32)


def draw_expert_ids(key, part):
    groups = LAYERS * MICRO * REPS
    block_rows = TOK_DEV // 2
    blocks = TOKENS // block_rows
    group_key = jax.random.fold_in(key, 7101)
    hot_all = jax.random.randint(jax.random.fold_in(group_key, 1), (groups,), 0, EXPERTS, dtype=jnp.int32)
    coin = jax.random.randint(jax.random.fold_in(group_key, 2), (LAYERS, MICRO, REPS), 0, 2, dtype=jnp.int32)
    micro_index = jnp.arange(MICRO, dtype=jnp.int32)[None, :, None]
    aligned_all = jnp.logical_or(coin == 1, micro_index == 0).reshape(groups)
    block_keys = jax.random.split(jax.random.fold_in(key, 7102), groups * blocks)
    hot_blocks = jnp.repeat(hot_all, blocks)
    aligned_blocks = jnp.repeat(aligned_all, blocks)
    result = jax.vmap(route_block)(block_keys, hot_blocks, aligned_blocks)
    return result.reshape(LAYERS, MICRO, REPS, TOKENS, TOP).astype(jnp.int32)


def level_of(rng, shape, cuts, low, largest):
    loudness = 1.0
    for axis_at, blocks in cuts:
        draws = jax.random.uniform(jax.random.fold_in(jax.random.fold_in(rng, 6), axis_at), (blocks,), jnp.float32, low / len(cuts), largest / len(cuts))
        loudness = loudness * jnp.repeat(jnp.exp(draws), shape[axis_at] // blocks).reshape((-1,) + (1,) * (len(shape) - 1 - axis_at))
    return loudness


def normal_values(stream_key, extent, width, most, pieces=(), held_as=jnp.bfloat16):
    entries = jax.random.normal(stream_key, extent, jnp.float32) * width
    if len(pieces) > 0:
        entries = level_of(stream_key, extent, pieces, -0.22, 0.18) * entries
    return jnp.clip(entries, min=-most, max=most).astype(held_as)


def setup_inputs(seed: int = 0) -> dict:
    splits = jax.random.split(jax.random.key(seed), 7)
    return {
        "tokens": normal_values(splits[0], (MICRO, REPS, TOKENS, D), 1.0, 6.0, ((2, 8),)),
        "expert_ids": draw_expert_ids(jax.random.fold_in(splits[6], 71), 0),
        "router_weight": normal_values(splits[2], (LAYERS, REPS, D, EXPERTS), (D // 4) ** -0.5, 0.375, ((0, 4),), jnp.float32),
        "w_gate": normal_values(splits[3], (LAYERS, N_EXPERT, D, FF), D ** -0.5, 0.1875, ((0, 4), (1, 8))),
        "w_up": normal_values(splits[4], (LAYERS, N_EXPERT, D, FF), D ** -0.5, 0.1875, ((0, 4), (1, 8))),
        "w_down": normal_values(splits[5], (LAYERS, N_EXPERT, FF, D), FF ** -0.5, 0.125, ((0, 4), (1, 8))),
    }


def normalize(hidden):
    values = hidden.astype(jnp.float32)
    return (values * lax.rsqrt(lax.optimization_barrier(jnp.mean(values * values, axis=-1, keepdims=True)) + 1e-06)).astype(jnp.bfloat16)

def expert_rows(inputs, gate_mat, up_mat, down_mat):
    gate_val = jnp.dot(inputs, gate_mat, preferred_element_type=jnp.float32)
    up_val = jnp.dot(inputs, up_mat, preferred_element_type=jnp.float32)
    inner = (jax.nn.silu(gate_val) * up_val).astype(jnp.bfloat16)
    return jnp.dot(inner, down_mat, preferred_element_type=jnp.float32).astype(jnp.bfloat16)

def reference(tokens, expert_ids, router_weight, w_gate, w_up, w_down):
    limit = MICRO * N_EXPERT * 2 * CAP
    hidden = tokens
    layer_list = []
    for layer in range(LAYERS):
        normed = normalize(hidden)
        logits = jnp.einsum('mrtd,rde->mrte', normed.astype(jnp.float32), router_weight[layer], precision=lax.Precision.HIGHEST)
        scores = jax.nn.sigmoid(logits)
        chosen = expert_ids[layer]
        picked = jnp.take_along_axis(scores, chosen, axis=-1)
        gates = picked / lax.optimization_barrier(jnp.sum(picked, axis=-1, keepdims=True))
        gate_layer = w_gate[layer]
        up_layer = w_up[layer]
        down_layer = w_down[layer]

        def one_replica(replica):
            rows_rep = lax.dynamic_index_in_dim(normed, replica, 1, keepdims=False).reshape(MICRO * TOKENS, D)
            ids_rep = lax.dynamic_index_in_dim(chosen, replica, 1, keepdims=False).reshape(-1)
            gates_rep = lax.dynamic_index_in_dim(gates, replica, 1, keepdims=False).reshape(-1)

            def one_expert(expert):
                member = ids_rep == expert
                order = jnp.argsort(jnp.where(member, 0, 1).astype(jnp.int32), stable=True)[:limit].astype(jnp.int32)
                source = (order // 2).astype(jnp.int32)
                instance = (replica * EXPERTS + expert).astype(jnp.int32)
                output = expert_rows(rows_rep[source], gate_layer[instance], up_layer[instance], down_layer[instance])
                weight = jnp.where(member[order], gates_rep[order], jnp.zeros_like(gates_rep[order]))
                return (source, weight[:, None] * output.astype(jnp.float32))
            sources, terms = lax.map(one_expert, jnp.arange(EXPERTS, dtype=jnp.int32))
            combined = jnp.zeros((MICRO * TOKENS, D), jnp.float32).at[sources.reshape(-1)].add(terms.reshape(-1, D))
            return combined.reshape(MICRO, TOKENS, D)
        combined = lax.map(one_replica, jnp.arange(REPS, dtype=jnp.int32))
        hidden = (hidden.astype(jnp.float32) + jnp.transpose(combined, (1, 0, 2, 3))).astype(jnp.bfloat16)
        layer_list.append(hidden)
    return jnp.stack(layer_list)
```

```python
import jax
import jax.numpy as jnp
from jax import lax
from jax.experimental import pallas as pl
from jax.experimental.pallas import tpu as pltpu
from jax.sharding import PartitionSpec as P

CAP = 4
VMEM = pl.BlockSpec(memory_space=pltpu.VMEM)
SMEM = pl.BlockSpec(memory_space=pltpu.SMEM)
HBM = pl.BlockSpec(memory_space=pl.ANY)


def norm_rows(x):
    values = x.astype(jnp.float32)
    scale = lax.rsqrt(jnp.mean(values * values, axis=-1, keepdims=True) + 1e-06)
    return (values * scale).astype(jnp.bfloat16)


def route_kernel(ids_ref, placing_ref, target_ref, *, experts, block_rows):
    replicas, rows, _ = ids_ref.shape
    share = rows // block_rows * CAP
    row = lax.broadcasted_iota(jnp.int32, (rows, rows), 0)
    col = lax.broadcasted_iota(jnp.int32, (rows, rows), 1)
    earlier = jnp.logical_and(col < row, col // block_rows == row // block_rows).astype(jnp.bfloat16)
    expert_range = lax.broadcasted_iota(jnp.int32, (rows, experts), 1)
    block_start = lax.broadcasted_iota(jnp.int32, (rows, 1), 0) // block_rows * CAP
    slot_range = lax.broadcasted_iota(jnp.int32, (rows, experts * share), 1)
    for r in range(replicas):
        ids = ids_ref[r]
        named = [(ids[:, k : k + 1] == expert_range).astype(jnp.float32) for k in range(2)]
        counts = jnp.dot(
            earlier, (named[0] + named[1]).astype(jnp.bfloat16), preferred_element_type=jnp.float32
        )
        targets = []
        for k in range(2):
            rank = jnp.sum(named[k] * counts, axis=-1, keepdims=True).astype(jnp.int32)
            targets.append(ids[:, k : k + 1] * share + block_start + rank)
        placed = jnp.logical_or(slot_range == targets[0], slot_range == targets[1])
        placing_ref[r] = placed.astype(jnp.float32).T.astype(jnp.bfloat16)
        target_ref[r] = jnp.concatenate(targets, axis=1)


def prepare_kernel(x_ref, placing_ref, out_ref):
    replicas = x_ref.shape[0]
    slots = placing_ref.shape[1]
    for r in range(replicas):
        normed = norm_rows(x_ref[r])
        out_ref[r * slots : (r + 1) * slots] = jnp.dot(
            placing_ref[r], normed, preferred_element_type=jnp.float32
        ).astype(jnp.bfloat16)


def gates_kernel(x_ref, router_ref, ids_ref, target_ref, mix_ref, *, slots):
    replicas, rows, _ = x_ref.shape
    experts = router_ref.shape[2]
    expert_range = lax.broadcasted_iota(jnp.int32, (rows, experts), 1)
    slot_range = lax.broadcasted_iota(jnp.int32, (rows, slots), 1)
    for r in range(replicas):
        normed = norm_rows(x_ref[r])
        logits = jnp.dot(
            normed.astype(jnp.float32),
            router_ref[r],
            precision=lax.Precision.HIGHEST,
            preferred_element_type=jnp.float32,
        )
        scores = 1.0 / (1.0 + jnp.exp(-logits))
        ids = ids_ref[r]
        picked = [
            jnp.sum(jnp.where(ids[:, k : k + 1] == expert_range, scores, 0.0), axis=-1, keepdims=True)
            for k in range(2)
        ]
        total = picked[0] + picked[1]
        target = target_ref[r]
        mix = sum(
            jnp.where(slot_range == target[:, k : k + 1], picked[k] / total, 0.0) for k in range(2)
        )
        high = mix.astype(jnp.bfloat16)
        mix_ref[r, :rows] = high
        mix_ref[r, rows:] = (mix - high.astype(jnp.float32)).astype(jnp.bfloat16)


def combine_kernel(section_ref, x_ref, mix_ref, answers_ref, kept_ref, out_ref, *, layer):
    replicas, rows, _ = x_ref.shape
    slots = mix_ref.shape[2]
    active = section_ref[0] == layer
    for r in range(replicas):
        both = jnp.dot(
            mix_ref[r], answers_ref[r * slots : (r + 1) * slots], preferred_element_type=jnp.float32
        )
        result = (x_ref[r].astype(jnp.float32) + (both[:rows] + both[rows:])).astype(jnp.bfloat16)
        out_ref[r] = jnp.where(active, result, kept_ref[r])


def expert_kernel(
    section_ref, rows_ref, gate_hbm, up_hbm, down_hbm, out_ref,
    gate_buf, up_buf, down_buf, inner_buf, sems, *, layer, chunk, out_chunk,
):
    width, hidden = gate_hbm.shape
    total = rows_ref.shape[0]
    row_step = min(total, 256)
    pieces = hidden // chunk
    out_pieces = width // out_chunk

    @pl.when(section_ref[0] == layer)
    def _():
        copies = []
        for j in range(pieces):
            part = pl.ds(j * chunk, chunk)
            first = pltpu.make_async_copy(gate_hbm.at[:, part], gate_buf.at[:, part], sems.at[0, j])
            second = pltpu.make_async_copy(up_hbm.at[:, part], up_buf.at[:, part], sems.at[1, j])
            first.start()
            second.start()
            copies.append((first, second))
        down_copies = []
        for j in range(out_pieces):
            part = pl.ds(j * out_chunk, out_chunk)
            copy = pltpu.make_async_copy(down_hbm.at[:, part], down_buf.at[:, part], sems.at[2, j])
            copy.start()
            down_copies.append(copy)
        for j in range(pieces):
            copies[j][0].wait()
            copies[j][1].wait()
            part = slice(j * chunk, (j + 1) * chunk)
            for i in range(0, total, row_step):
                block = rows_ref[i : i + row_step]
                gate_val = jnp.dot(block, gate_buf[:, part], preferred_element_type=jnp.float32)
                up_val = jnp.dot(block, up_buf[:, part], preferred_element_type=jnp.float32)
                act = gate_val / (1.0 + jnp.exp(-gate_val)) * up_val
                inner_buf[i : i + row_step, part] = act.astype(jnp.bfloat16)
        for j in range(out_pieces):
            down_copies[j].wait()
            part = slice(j * out_chunk, (j + 1) * out_chunk)
            for i in range(0, total, row_step):
                out_ref[i : i + row_step, part] = jnp.dot(
                    inner_buf[i : i + row_step], down_buf[:, part], preferred_element_type=jnp.float32
                ).astype(jnp.bfloat16)


def per_device(tokens, expert_ids, router_weight, w_gate, w_up, w_down):
    batches, replicas, tok_dev, width = tokens.shape
    experts = router_weight.shape[3]
    hidden = w_gate.shape[3]
    sections = lax.axis_size("section")
    section = lax.axis_index("section").astype(jnp.int32).reshape(1)
    rows = batches * tok_dev
    block_rows = tok_dev // 2
    share = rows // block_rows * CAP
    slots = experts * share
    gate_mat, up_mat, down_mat = w_gate[0, 0], w_up[0, 0], w_down[0, 0]
    router = router_weight[0]
    ids = jnp.swapaxes(expert_ids[0], 0, 1).reshape(replicas, rows, 2)
    chunk, out_chunk = 256, 256

    placing, target = pl.pallas_call(
        lambda *refs: route_kernel(*refs, experts=experts, block_rows=block_rows),
        out_shape=(
            jax.ShapeDtypeStruct((replicas, slots, rows), jnp.bfloat16),
            jax.ShapeDtypeStruct((replicas, rows, 2), jnp.int32),
        ),
        in_specs=[VMEM],
        out_specs=(VMEM, VMEM),
        name="route",
    )(ids)

    def prepare(x):
        return pl.pallas_call(
            prepare_kernel,
            out_shape=jax.ShapeDtypeStruct((replicas * slots, width), jnp.bfloat16),
            in_specs=[VMEM, VMEM],
            out_specs=VMEM,
            name="prepare",
        )(x, placing)

    def gates(x):
        return pl.pallas_call(
            lambda *refs: gates_kernel(*refs, slots=slots),
            out_shape=jax.ShapeDtypeStruct((replicas, 2 * rows, slots), jnp.bfloat16),
            in_specs=[VMEM] * 4,
            out_specs=VMEM,
            name="gates",
        )(x, router, ids, target)

    def expert(received, layer):
        total = received.shape[0]
        return pl.pallas_call(
            lambda *refs: expert_kernel(*refs, layer=layer, chunk=chunk, out_chunk=out_chunk),
            out_shape=jax.ShapeDtypeStruct((total, width), jnp.bfloat16),
            in_specs=[SMEM, VMEM, HBM, HBM, HBM],
            out_specs=VMEM,
            scratch_shapes=[
                pltpu.VMEM((width, hidden), jnp.bfloat16),
                pltpu.VMEM((width, hidden), jnp.bfloat16),
                pltpu.VMEM((hidden, width), jnp.bfloat16),
                pltpu.VMEM((total, hidden), jnp.bfloat16),
                pltpu.SemaphoreType.DMA((3, max(hidden // chunk, width // out_chunk))),
            ],
            compiler_params=pltpu.CompilerParams(vmem_limit_bytes=40 << 20),
            name="expert",
        )(section, received, gate_mat, up_mat, down_mat)

    def combine(x, mix, answers, kept, layer):
        return pl.pallas_call(
            lambda *refs: combine_kernel(*refs, layer=layer),
            out_shape=jax.ShapeDtypeStruct((replicas, rows, width), jnp.bfloat16),
            in_specs=[SMEM] + [VMEM] * 4,
            out_specs=VMEM,
            name="combine",
        )(section, x, mix, answers, kept)

    def exchange(array):
        return lax.all_to_all(array, "expert", split_axis=0, concat_axis=0, tiled=True)

    current = jnp.swapaxes(tokens, 0, 1).reshape(replicas, rows, width)
    kept = current
    for layer in range(sections):
        received = exchange(prepare(current))
        mix = gates(current)
        answers = exchange(expert(received, layer))
        kept = combine(current, mix, answers, kept, layer)
        if layer + 1 < sections:
            current = lax.ppermute(kept, "section", [(layer, layer + 1)])
    out = jnp.swapaxes(kept.reshape(replicas, batches, tok_dev, width), 0, 1)
    return out[None]


def solution(mesh):
    in_specs = (
        P(None, None, "expert", None),
        P("section", None, None, "expert", None),
        P("section", None, None, None),
        P("section", "expert", None, None),
        P("section", "expert", None, None),
        P("section", "expert", None, None),
    )
    out_specs = P("section", None, None, "expert", None)
    return jax.shard_map(
        per_device, mesh=mesh, in_specs=in_specs, out_specs=out_specs, check_vma=False
    )
```

```python
import jax
import jax.numpy as jnp
from jax import lax
from jax.experimental import pallas as pl
from jax.experimental.pallas import tpu as pltpu
from jax.sharding import PartitionSpec as P

CAP = 4
CHUNK = 256
UNITS = 1
VMEM = pl.BlockSpec(memory_space=pltpu.VMEM)
SMEM = pl.BlockSpec(memory_space=pltpu.SMEM)


def near(array):
    return pltpu.with_memory_space_constraint(array, pltpu.VMEM)


def norm_rows(x):
    values = x.astype(jnp.float32)
    scale = lax.rsqrt(jnp.mean(values * values, axis=-1, keepdims=True) + 1e-06)
    return (values * scale).astype(jnp.bfloat16)


def unit_of(section_ref, step, units):
    return jnp.clip(step - section_ref[0], 0, units - 1)


def is_active(section_ref, step, units):
    return jnp.logical_and(step >= section_ref[0], step - section_ref[0] < units)


def start_kernel(
    section_ref, ids_ref, tokens_ref, placing_ref, target_ref, x_ref, out_ref, *, experts, units
):
    _, batches, replicas, _, tok_dev = ids_ref.shape
    span = batches // units
    rows = span * tok_dev
    block_rows = tok_dev // 2
    share = rows // block_rows * CAP
    slots = experts * share
    row = lax.broadcasted_iota(jnp.int32, (rows, rows), 0)
    col = lax.broadcasted_iota(jnp.int32, (rows, rows), 1)
    earlier = jnp.logical_and(row < col, row // block_rows == col // block_rows)
    earlier = earlier.astype(jnp.float32).astype(jnp.bfloat16)
    expert_range = lax.broadcasted_iota(jnp.int32, (experts, rows), 0)
    block_start = lax.broadcasted_iota(jnp.int32, (1, rows), 1) // block_rows * CAP
    slot_range = lax.broadcasted_iota(jnp.int32, (slots, rows), 0)
    for u in range(units):
        for r in range(replicas):
            members = range(u * span, (u + 1) * span)
            ids = jnp.concatenate([ids_ref[0, m, r] for m in members], axis=1)
            named = [(ids[k : k + 1] == expert_range).astype(jnp.float32) for k in range(2)]
            counts = jnp.dot(
                (named[0] + named[1]).astype(jnp.bfloat16), earlier, preferred_element_type=jnp.float32
            )
            targets = []
            for k in range(2):
                rank = jnp.sum(named[k] * counts, axis=0, keepdims=True).astype(jnp.int32)
                targets.append(ids[k : k + 1] * share + block_start + rank)
                target_ref[u, r, k : k + 1] = targets[k]
            placed = jnp.logical_or(slot_range == targets[0], slot_range == targets[1])
            placing = placed.astype(jnp.float32).astype(jnp.bfloat16)
            placing_ref[u, r] = placing
            x = jnp.concatenate([tokens_ref[m, r] for m in members], axis=0)
            x_ref[u, r] = x
            if u == 0:
                out_ref[r * slots : (r + 1) * slots] = jnp.dot(
                    placing, norm_rows(x), preferred_element_type=jnp.float32
                ).astype(jnp.bfloat16)


def prepare_kernel(section_ref, incoming_ref, tokens_ref, placing_ref, x_ref, out_ref, *, step):
    units, replicas, slots, _ = placing_ref.shape
    unit = unit_of(section_ref, step, units)
    for r in range(replicas):
        x = incoming_ref[r]
        if step < units:
            x = jnp.where(section_ref[0] == 0, tokens_ref[unit, r], x)
        x_ref[r] = x
        out_ref[r * slots : (r + 1) * slots] = jnp.dot(
            placing_ref[unit, r], norm_rows(x), preferred_element_type=jnp.float32
        ).astype(jnp.bfloat16)


def mix_rows(x, router, ids, targets, slots):
    rows = x.shape[0]
    experts = router.shape[0]
    expert_range = lax.broadcasted_iota(jnp.int32, (experts, rows), 0)
    slot_range = lax.broadcasted_iota(jnp.int32, (slots, rows), 0)
    logits = lax.dot_general(
        router,
        norm_rows(x).astype(jnp.float32),
        (((1,), (1,)), ((), ())),
        precision=lax.Precision.HIGHEST,
        preferred_element_type=jnp.float32,
    )
    scores = 1.0 / (1.0 + jnp.exp(-logits))
    picked = [
        jnp.sum(jnp.where(ids[k : k + 1] == expert_range, scores, 0.0), axis=0, keepdims=True)
        for k in range(2)
    ]
    total = picked[0] + picked[1]
    return sum(
        jnp.where(slot_range == targets[k : k + 1], picked[k] / total, 0.0) for k in range(2)
    ).T


def expert_kernel(
    section_ref, rows_ref, gate_ref, up_ref, down_ref, x_ref, router_ref, ids_ref, target_ref,
    out_ref, mix_ref, inner_ref, *, step,
):
    width, hidden = gate_ref.shape
    total = rows_ref.shape[0]
    row_step = min(total, 256)
    units, replicas, _, _ = target_ref.shape
    span = ids_ref.shape[1] // units
    rows = x_ref.shape[1]
    slots = mix_ref.shape[2]
    unit = unit_of(section_ref, step, units)

    def run_rows(start):
        block = rows_ref[pl.ds(start, row_step)]
        for j in range(0, hidden, CHUNK):
            part = slice(j, j + CHUNK)
            gate_val = jnp.dot(block, gate_ref[:, part], preferred_element_type=jnp.float32)
            up_val = jnp.dot(block, up_ref[:, part], preferred_element_type=jnp.float32)
            inner_ref[:, part] = (gate_val / (1.0 + jnp.exp(-gate_val)) * up_val).astype(jnp.bfloat16)
        for j in range(0, width, CHUNK):
            part = slice(j, j + CHUNK)
            out_ref[pl.ds(start, row_step), part] = jnp.dot(
                inner_ref[...], down_ref[:, part], preferred_element_type=jnp.float32
            ).astype(jnp.bfloat16)

    @pl.when(is_active(section_ref, step, units))
    def _():
        for r in range(replicas):
            ids = jnp.concatenate([ids_ref[0, unit * span + m, r] for m in range(span)], axis=1)
            mix = mix_rows(x_ref[r], router_ref[0, r], ids, target_ref[unit, r], slots)
            high = mix.astype(jnp.bfloat16)
            mix_ref[r, :rows] = high
            mix_ref[r, rows:] = (mix - high.astype(jnp.float32)).astype(jnp.bfloat16)
        if total == row_step:
            run_rows(0)
        else:

            @pl.loop(0, total // row_step)
            def _(i):
                run_rows(pl.multiple_of(i * row_step, row_step))


def combine_kernel(section_ref, x_ref, mix_ref, answers_ref, kept_ref, out_ref, *refs, step, last):
    replicas, rows, _ = x_ref.shape
    units = kept_ref.shape[0]
    slots = mix_ref.shape[2]
    unit = unit_of(section_ref, step, units)
    active = is_active(section_ref, step, units)
    for r in range(replicas):
        both = jnp.dot(
            mix_ref[r], answers_ref[r * slots : (r + 1) * slots], preferred_element_type=jnp.float32
        )
        result = (x_ref[r].astype(jnp.float32) + (both[:rows] + both[rows:])).astype(jnp.bfloat16)
        for u in range(units):
            here = jnp.logical_and(active, unit == u)
            out_ref[u, r] = jnp.where(here, result, kept_ref[u, r])
        if not last:
            refs[0][r] = result


def per_device(tokens, expert_ids, router_weight, w_gate, w_up, w_down):
    batches, replicas, tok_dev, width = tokens.shape
    experts = router_weight.shape[3]
    hidden = w_gate.shape[3]
    sections = lax.axis_size("section")
    section = lax.axis_index("section").astype(jnp.int32).reshape(1)
    units = UNITS
    rows = batches // units * tok_dev
    slots = experts * (rows // (tok_dev // 2) * CAP)
    router = jnp.swapaxes(router_weight, 2, 3)
    ids = jnp.swapaxes(expert_ids, 3, 4)
    mats = tuple(w[0, 0] for w in (w_gate, w_up, w_down))
    params = pltpu.CompilerParams(vmem_limit_bytes=16 << 20)

    def call(kernel, name, args, shapes, scratch=(), **static):
        outs = tuple(
            jax.ShapeDtypeStruct(s.shape, s.dtype) if far else pltpu.VMEM(s.shape, s.dtype)
            for s, far in shapes
        )
        return pl.pallas_call(
            lambda *refs: kernel(*refs, **static),
            out_shape=outs,
            in_specs=[SMEM if a is section else VMEM for a in args],
            out_specs=(VMEM,) * len(outs),
            scratch_shapes=scratch,
            compiler_params=params,
            cost_estimate=pl.CostEstimate(flops=10**10, bytes_accessed=10**8, transcendentals=0),
            name=name,
        )(*(a if a is section or name == "start" else near(a) for a in args))

    def shape(*dims, dtype=jnp.bfloat16, far=False):
        return (jax.ShapeDtypeStruct(dims, dtype), far)

    def exchange(array):
        return lax.all_to_all(array, "expert", split_axis=0, concat_axis=0, tiled=True)

    placing, target, staged, outgoing = call(
        start_kernel,
        "start",
        (section, ids, tokens),
        (
            shape(units, replicas, slots, rows),
            shape(units, replicas, 2, rows, dtype=jnp.int32),
            shape(units, replicas, rows, width),
            shape(replicas * slots, width),
        ),
        experts=experts,
        units=units,
    )
    current, kept = staged[0], staged
    steps = sections + units - 1
    for step in range(steps):
        last = step + 1 == steps
        received = exchange(outgoing)
        total = received.shape[0]
        answers, mix = call(
            expert_kernel,
            "expert",
            (section, received, *mats, current, router, ids, target),
            (shape(total, width), shape(replicas, 2 * rows, slots)),
            scratch=[pltpu.VMEM((min(total, 256), hidden), jnp.bfloat16)],
            step=step,
        )
        outs = [shape(units, replicas, rows, width, far=last)]
        if not last:
            outs.append(shape(replicas, rows, width))
        kept, *result = call(
            combine_kernel,
            "combine",
            (section, current, mix, exchange(answers), kept),
            outs,
            step=step,
            last=last,
        )
        if not last:
            pairs = [(s, s + 1) for s in range(sections - 1) if 0 <= step - s < units]
            incoming = lax.ppermute(result[0], "section", pairs)
            current, outgoing = call(
                prepare_kernel,
                "prepare",
                (section, incoming, staged, placing),
                (shape(replicas, rows, width), shape(replicas * slots, width)),
                step=step + 1,
            )
    out = jnp.transpose(
        kept.reshape(units, replicas, batches // units, tok_dev, width), (0, 2, 1, 3, 4)
    )
    return out.reshape(1, batches, replicas, tok_dev, width)


def solution(mesh):
    in_specs = (
        P(None, None, "expert", None),
        P("section", None, None, "expert", None),
        P("section", None, None, None),
        P("section", "expert", None, None),
        P("section", "expert", None, None),
        P("section", "expert", None, None),
    )
    out_specs = P("section", None, None, "expert", None)
    return jax.shard_map(
        per_device, mesh=mesh, in_specs=in_specs, out_specs=out_specs, check_vma=False
    )
```

```python
import jax
import jax.numpy as jnp
from jax import lax
from jax.experimental import pallas as pl
from jax.experimental.pallas import tpu as pltpu
from jax.sharding import PartitionSpec as P

CAP = 4
CHUNK = 256
UNITS = 2
COST = pl.CostEstimate(flops=10**10, bytes_accessed=10**8, transcendentals=0)
VMEM = pl.BlockSpec(memory_space=pltpu.VMEM)
ANY = pl.BlockSpec(memory_space=pl.ANY)
SMEM = pl.BlockSpec(memory_space=pltpu.SMEM)


def norm_rows(x):
    values = x.astype(jnp.float32)
    scale = lax.rsqrt(jnp.mean(values * values, axis=-1, keepdims=True) + 1e-06)
    return (values * scale).astype(jnp.bfloat16)


def start_kernel(
    self_ref, ids_hbm, tokens_hbm, ids_ref, placing_ref, target_ref, x_ref, sems, id_sem,
    *, experts, paired,
):
    _, batches, replicas, _, tok_dev = ids_ref.shape
    units = x_ref.shape[0]
    span = batches // units
    rows = span * tok_dev
    block_rows = tok_dev // 2
    share = rows // block_rows * CAP
    slots = experts * share
    id_copy = pltpu.make_async_copy(ids_hbm, ids_ref, id_sem)
    id_copy.start()
    copies = {}
    for m in range(batches):
        for r in range(replicas):
            place = x_ref.at[m // span, r, pl.ds(m % span * tok_dev, tok_dev)]
            copies[m, r] = pltpu.make_async_copy(tokens_hbm.at[m, r], place, sems.at[m, r])
            copies[m, r].start()
    row = lax.broadcasted_iota(jnp.int32, (rows, rows), 0)
    col = lax.broadcasted_iota(jnp.int32, (rows, rows), 1)
    earlier = jnp.logical_and(row < col, row // block_rows == col // block_rows)
    earlier = earlier.astype(jnp.float32).astype(jnp.bfloat16)
    expert_range = lax.broadcasted_iota(jnp.int32, (experts, rows), 0)
    block_start = lax.broadcasted_iota(jnp.int32, (1, rows), 1) // block_rows * CAP
    slot_range = lax.broadcasted_iota(jnp.int32, (slots, rows), 0)
    id_copy.wait()
    for u in range(units):
        for r in range(replicas):
            ids = jnp.concatenate([ids_ref[0, u * span + m, r] for m in range(span)], axis=1)
            named = [(ids[k : k + 1] == expert_range).astype(jnp.float32) for k in range(2)]
            counts = jnp.dot(
                (named[0] + named[1]).astype(jnp.bfloat16), earlier, preferred_element_type=jnp.float32
            )
            targets = []
            place = ids
            if paired:
                place = jnp.bitwise_xor(ids, self_ref[0])
                place = (place & 1) * (experts // 2) + (place >> 1)
            for k in range(2):
                rank = jnp.sum(named[k] * counts, axis=0, keepdims=True).astype(jnp.int32)
                targets.append(place[k : k + 1] * share + block_start + rank)
                target_ref[u, r, k : k + 1] = targets[k]
            placed = jnp.logical_or(slot_range == targets[0], slot_range == targets[1])
            placing_ref[u, r] = placed.astype(jnp.float32).astype(jnp.bfloat16)
    for copy in copies.values():
        copy.wait()


def prepare_kernel(x_ref, placing_ref, *out_refs, unit):
    _, replicas, slots, _ = placing_ref.shape
    for r in range(replicas):
        outgoing = jnp.dot(
            placing_ref[unit, r], norm_rows(x_ref[r]), preferred_element_type=jnp.float32
        ).astype(jnp.bfloat16)
        if len(out_refs) == 1:
            out_refs[0][r * slots : (r + 1) * slots] = outgoing
        else:
            out_refs[0][...] = outgoing[: slots // 2]
            out_refs[1][...] = outgoing[slots // 2 :]


def mix_rows(x, router, ids, targets, slots):
    rows = x.shape[0]
    experts = router.shape[0]
    expert_range = lax.broadcasted_iota(jnp.int32, (experts, rows), 0)
    slot_range = lax.broadcasted_iota(jnp.int32, (slots, rows), 0)
    logits = lax.dot_general(
        router,
        norm_rows(x).astype(jnp.float32),
        (((1,), (1,)), ((), ())),
        precision=lax.Precision.HIGHEST,
        preferred_element_type=jnp.float32,
    )
    scores = 1.0 / (1.0 + jnp.exp(-logits))
    picked = [
        jnp.sum(jnp.where(ids[k : k + 1] == expert_range, scores, 0.0), axis=0, keepdims=True)
        for k in range(2)
    ]
    total = picked[0] + picked[1]
    return sum(
        jnp.where(slot_range == targets[k : k + 1], picked[k] / total, 0.0) for k in range(2)
    ).T


def expert_kernel(*refs, unit, pieces):
    rows_refs, refs = refs[:pieces], refs[pieces:]
    gate_ref, up_ref, down_ref, x_ref, router_ref, ids_ref, target_ref, *refs = refs
    out_refs, (mix_ref, inner_ref) = refs[:pieces], refs[pieces:]
    width, hidden = gate_ref.shape
    length = rows_refs[0].shape[0]
    row_step = min(length, 256)
    units, replicas, _, _ = target_ref.shape
    span = ids_ref.shape[1] // units
    rows = x_ref.shape[1]
    slots = mix_ref.shape[2]
    for r in range(replicas):
        ids = jnp.concatenate([ids_ref[0, unit * span + m, r] for m in range(span)], axis=1)
        mix = mix_rows(x_ref[r], router_ref[0, r], ids, target_ref[unit, r], slots)
        high = mix.astype(jnp.bfloat16)
        mix_ref[r, :rows] = high
        mix_ref[r, rows:] = (mix - high.astype(jnp.float32)).astype(jnp.bfloat16)

    def run_rows(start):
        part_rows = pl.ds(start, row_step)
        block = jnp.concatenate([ref[part_rows] for ref in rows_refs], axis=0)
        for j in range(0, hidden, CHUNK):
            part = slice(j, j + CHUNK)
            gate_val = jnp.dot(block, gate_ref[:, part], preferred_element_type=jnp.float32)
            up_val = jnp.dot(block, up_ref[:, part], preferred_element_type=jnp.float32)
            inner_ref[:, part] = (gate_val / (1.0 + jnp.exp(-gate_val)) * up_val).astype(jnp.bfloat16)
        for j in range(0, width, CHUNK):
            part = slice(j, j + CHUNK)
            result = jnp.dot(
                inner_ref[...], down_ref[:, part], preferred_element_type=jnp.float32
            ).astype(jnp.bfloat16)
            for p, ref in enumerate(out_refs):
                ref[part_rows, part] = result[p * row_step : (p + 1) * row_step]

    if length == row_step:
        run_rows(0)
    else:

        @pl.loop(0, length // row_step)
        def _(i):
            run_rows(pl.multiple_of(i * row_step, row_step))


def combine_kernel(x_ref, mix_ref, *refs):
    *answer_refs, out_ref = refs
    replicas, rows, _ = x_ref.shape
    slots = mix_ref.shape[2]
    for r in range(replicas):
        first = answer_refs[0][r * slots : (r + 1) * slots]
        if len(answer_refs) > 1:
            near_rows = slots // 2 // (len(answer_refs) - 1)
            first = jnp.concatenate(
                [ref[:near_rows] for ref in answer_refs[:-1]] + [answer_refs[-1][...]], axis=0
            )
        both = jnp.dot(mix_ref[r], first, preferred_element_type=jnp.float32)
        out_ref[r] = (x_ref[r].astype(jnp.float32) + (both[:rows] + both[rows:])).astype(jnp.bfloat16)


def per_device(tokens, expert_ids, router_weight, w_gate, w_up, w_down):
    batches, replicas, tok_dev, width = tokens.shape
    experts = router_weight.shape[3]
    hidden = w_gate.shape[3]
    sections = lax.axis_size("section")
    section = lax.axis_index("section")
    units = UNITS if batches % UNITS == 0 else 1
    rows = batches // units * tok_dev
    slots = experts * (rows // (tok_dev // 2) * CAP)
    router = jnp.swapaxes(router_weight, 2, 3)
    ids_far = jnp.swapaxes(expert_ids, 3, 4)
    mats = tuple(w[0, 0] for w in (w_gate, w_up, w_down))

    peers = lax.axis_size("expert")
    paired = replicas == 1 and peers == experts == 8
    self_index = lax.axis_index("expert").astype(jnp.int32).reshape(1)
    share = slots // experts

    def call(kernel, name, args, outs, scratch=(), far=False, **static):
        space = pltpu.HBM if far else pltpu.VMEM
        return pl.pallas_call(
            lambda *refs: kernel(*refs, **static),
            out_shape=outs,
            in_specs=[SMEM if a is self_index else ANY if far else VMEM for a in args],
            out_specs=jax.tree.map(lambda _: VMEM, outs),
            scratch_shapes=scratch,
            compiler_params=pltpu.CompilerParams(vmem_limit_bytes=16 << 20),
            cost_estimate=COST,
            name=name,
        )(*(a if a is self_index else pltpu.with_memory_space_constraint(a, space) for a in args))

    def exchange(array):
        return lax.all_to_all(array, "expert", split_axis=0, concat_axis=0, tiled=True)

    def flip(array, bits):
        return lax.ppermute(array, "expert", [(i, i ^ bits) for i in range(peers)])

    def flip_all(parts):
        moved = {c: flip(parts[c], 2 * c) for c in (3, 1, 2)}
        return [parts[0]] + [moved[c] for c in range(1, len(parts))]

    def out_array(*dims):
        return pltpu.VMEM(dims, jnp.bfloat16)

    def block(x, unit):
        if paired:
            same, other = call(
                prepare_kernel,
                "prepare",
                (x, placing),
                (out_array(slots // 2, width),) * 2,
                unit=unit,
            )
            same = same.reshape(experts // 2, share, width)
            other = flip(other, 1).reshape(experts // 2, share, width)
            received = flip_all(
                [jnp.concatenate([same[c], other[c]], axis=0) for c in range(experts // 2)]
            )
        else:
            outgoing = call(
                prepare_kernel, "prepare", (x, placing), (out_array(replicas * slots, width),), unit=unit
            )[0]
            received = [exchange(outgoing)]
        length = received[0].shape[0]
        pieces = len(received)
        *answers, mix = call(
            expert_kernel,
            "expert",
            (*received, *mats, x, router, ids, target),
            (out_array(length, width),) * pieces + (out_array(replicas, 2 * rows, slots),),
            scratch=[pltpu.VMEM((min(length, 256) * pieces, hidden), jnp.bfloat16)],
            unit=unit,
            pieces=pieces,
        )
        if paired:
            answers = flip_all(answers)
            answers.append(flip(jnp.concatenate([part[share:] for part in answers], axis=0), 1))
        else:
            answers = [exchange(answers[0])]
        return call(combine_kernel, "combine", (x, mix, *answers), out_array(replicas, rows, width))

    ids, placing, target, staged = call(
        start_kernel,
        "start",
        (self_index, ids_far, tokens),
        (
            pltpu.VMEM(ids_far.shape, jnp.int32),
            out_array(units, replicas, slots, rows),
            pltpu.VMEM((units, replicas, 2, rows), jnp.int32),
            out_array(units, replicas, rows, width),
        ),
        scratch=[pltpu.SemaphoreType.DMA((batches, replicas)), pltpu.SemaphoreType.DMA(())],
        far=True,
        experts=experts,
        paired=paired,
    )
    held = [staged[u] for u in range(units)]
    kept = list(held)
    for layer in range(sections):
        for unit in range(units):
            kept[unit] = lax.cond(
                section == layer,
                lambda x, old, unit=unit: block(x, unit),
                lambda x, old: old,
                held[unit],
                kept[unit],
            )
        if layer + 1 < sections:
            pairs = [(layer, layer + 1)]
            held = [lax.ppermute(kept[unit], "section", pairs) for unit in range(units)]
            held[0], _ = lax.optimization_barrier((held[0], kept[-1]))
    out = jnp.stack(kept).reshape(units, replicas, batches // units, tok_dev, width)
    return jnp.swapaxes(out, 1, 2).reshape(1, batches, replicas, tok_dev, width)


def solution(mesh):
    in_specs = (
        P(None, None, "expert", None),
        P("section", None, None, "expert", None),
        P("section", None, None, None),
        P("section", "expert", None, None),
        P("section", "expert", None, None),
        P("section", "expert", None, None),
    )
    out_specs = P("section", None, None, "expert", None)
    return jax.shard_map(
        per_device, mesh=mesh, in_specs=in_specs, out_specs=out_specs, check_vma=False
    )
```
